32 devices in a mesh: rep: 1 (over z), r: 4 (over y), s: 8 (over x, core).
Axes of the slice: x: 4, y: 4, z: 1, core: 2. Of those that a mesh axis runs over, the one named last changes fastest.
The devices are a block of a 4x4x8 slice.
Arguments:
- x: bfloat16 [32, 2048, 1024], P(('rep', 'r', 's'))
- dy: bfloat16 [32, 2048, 1024], P(('rep', 'r', 's'))
- w_gate: bfloat16 [2, 1024, 2560], P(None, 's')
- w_up: bfloat16 [2, 1024, 2560], P(None, 's')
- w_down: bfloat16 [2, 2560, 1024], P(None, 's')
- m_w_gate: float32 [2, 1024, 2560], P(None, 's')
- m_w_up: float32 [2, 1024, 2560], P(None, 's')
- m_w_down: float32 [2, 2560, 1024], P(None, 's')
- v_w_gate: float32 [2, 1024, 2560], P(None, 's')
- v_w_up: float32 [2, 1024, 2560], P(None, 's')
- v_w_down: float32 [2, 2560, 1024], P(None, 's')
Outputs:
- output 1: bfloat16 [2, 1024, 2560], P('rep', 's')
- output 2: bfloat16 [2, 1024, 2560], P('rep', 's')
- output 3: bfloat16 [2, 2560, 1024], P('rep', 's')
- output 4: float32 [2, 1024, 2560], P('rep', 's')
- output 5: float32 [2, 1024, 2560], P('rep', 's')
- output 6: float32 [2, 2560, 1024], P('rep', 's')
- output 7: float32 [2, 1024, 2560], P('rep', 's')
- output 8: float32 [2, 1024, 2560], P('rep', 's')
- output 9: float32 [2, 2560, 1024], P('rep', 's')
All inputs are finite; a program needn't handle non-finite values.
Results may differ from the reference program's by a relative error of at most 0.022.
Values are sent between devices in bfloat16 or wider.
A program may use at most 768 MiB of HBM per device.

```python
import jax
import jax.numpy as jnp
from jax import lax

SEQUENCES = 32
TOKENS = 2048
D = 1024
FF = 2560
LAYERS = 2
NAMES = ("w_gate", "w_up", "w_down")
SHAPES = {"w_gate": (LAYERS, D, FF), "w_up": (LAYERS, D, FF), "w_down": (LAYERS, FF, D)}


def bump(key, n, height):
    away = (jnp.arange(n, dtype=jnp.int32) - jax.random.randint(key, (), 0, n, jnp.int32)) % n
    return jnp.where(away < n // 8, height, 1.0)


def together(key, own, strength):
    shared = jax.random.normal(key, own.shape[1:], jnp.float32)
    return (own + strength * shared) * lax.rsqrt(1 + strength * strength)


def setup_inputs(seed: int = 0, part: int = 0) -> dict:
    kx, kdy, ka, kb, kz, kf, kh, kl, *keys = jax.random.split(jax.random.key(seed), 8 + 3 * len(NAMES))
    kx, kdy, ka, kb = (jax.random.fold_in(k, part) for k in (kx, kdy, ka, kb))
    kw, km, kv = (keys[i::3] for i in range(3))
    shape = (SEQUENCES, TOKENS, D)
    much_x, much_dy = jax.random.uniform(kz, (2,), jnp.float32, 0.0, 1.0)
    loud = 2.0 ** jax.random.uniform(jax.random.fold_in(kz, 1), (), jnp.float32, -1.0, 2.0)
    layers = 2.0 ** jax.random.uniform(kl, (LAYERS, 1, 1), jnp.float32, -1.0, 1.0)
    x = together(ka, jax.random.normal(kx, shape, jnp.float32), much_x) * bump(kf, D, 4.0)
    dy = together(kb, jax.random.normal(kdy, shape, jnp.float32), much_dy)
    drawn = {"x": x.astype(jnp.bfloat16), "dy": (loud * dy * (SEQUENCES * TOKENS) ** -0.5).astype(jnp.bfloat16)}
    for key, name in zip(kw, NAMES, strict=True):
        w = jax.random.normal(key, SHAPES[name], jnp.float32) * SHAPES[name][1] ** -0.5
        drawn[name] = (w * {"w_gate": 1.0, "w_up": bump(kh, FF, 4.0), "w_down": layers}[name]).astype(jnp.bfloat16)
    for key, name in zip(km, NAMES, strict=True):
        drawn[f"m_{name}"] = 0.1 * jax.random.normal(key, SHAPES[name], jnp.float32)
    for key, name in zip(kv, NAMES, strict=True):
        drawn[f"v_{name}"] = jax.random.uniform(key, SHAPES[name], jnp.float32, 0.005, 0.015)
    return drawn


def matmul(a, w):
    return jnp.dot(a, w, preferred_element_type=jnp.float32).astype(jnp.bfloat16)


def normed(h):
    wide = h.astype(jnp.float32)
    scale = lax.rsqrt(jnp.mean(wide**2, -1, keepdims=True) + 1e-6)
    return (wide * scale).astype(jnp.bfloat16)


def layer(h, w):
    a = normed(h)
    gate = jnp.dot(a, w["w_gate"], preferred_element_type=jnp.float32)
    up = jnp.dot(a, w["w_up"], preferred_element_type=jnp.float32)
    return h + matmul((jax.nn.silu(gate) * up).astype(jnp.bfloat16), w["w_down"])


def adamw(w, m, v, g):
    m = 0.9 * m + 0.1 * g
    v = 0.95 * v + 0.05 * g * g
    step = m * lax.rsqrt(v + 1e-8) + 0.1 * w
    return (w - 0.02 * step).astype(jnp.bfloat16), m, v


def clipped(gradients, sum_of_squares, count):
    factor = jnp.minimum(1.0, 0.5 * lax.rsqrt(sum_of_squares / count + 1e-30))
    return [g * factor for g in gradients]


def stack(weights, h):
    return lax.scan(lambda h, w: (layer(h, w), None), h, weights)[0]


def reference(x, dy, w_gate, w_up, w_down, m_w_gate, m_w_up, m_w_down, v_w_gate, v_w_up, v_w_down):
    weights = dict(zip(NAMES, (w_gate, w_up, w_down), strict=True))

    def take(so_far, sequence):
        h, by_y = sequence
        _, back = jax.vjp(lambda w: stack(w, h), weights)
        return jax.tree.map(lambda total, term: total + term.astype(jnp.float32), so_far, back(by_y)[0]), None

    none_yet = {name: jnp.zeros(w.shape, jnp.float32) for name, w in weights.items()}
    by_weights, _ = lax.scan(take, none_yet, (x, dy))
    gradients = [by_weights[name].astype(jnp.bfloat16).astype(jnp.float32) for name in NAMES]
    gradients = clipped(gradients, sum(jnp.sum(g * g) for g in gradients), sum(g.size for g in gradients))
    new = [
        adamw(w.astype(jnp.float32), m, v, g)
        for w, m, v, g in zip((w_gate, w_up, w_down), (m_w_gate, m_w_up, m_w_down), (v_w_gate, v_w_up, v_w_down), gradients, strict=True)
    ]
    return tuple(one[which] for which in range(3) for one in new)
```

```python
import functools

import jax
import jax.numpy as jnp
from jax import lax
from jax.experimental import pallas as pl
from jax.experimental.pallas import tpu as pltpu
from jax.sharding import PartitionSpec as P

MESH = pl.DeviceIdType.MESH
BF16, F32 = jnp.bfloat16, jnp.float32
ANY = pl.BlockSpec(memory_space=pl.ANY)
VMEM_LIMIT = 67_000_000
RING = 4


def adamw(w, m, v, g):
    m = 0.9 * m + 0.1 * g
    v = 0.95 * v + 0.05 * g * g
    step = m * lax.rsqrt(v + 1e-8) + 0.1 * w
    return (w - 0.02 * step).astype(jnp.bfloat16), m, v


def clipped(gradients, sum_of_squares, count):
    factor = jnp.minimum(1.0, 0.5 * lax.rsqrt(sum_of_squares / count + 1e-30))
    return [g * factor for g in gradients]


def scale_of(wide):
    return lax.rsqrt(jnp.mean(wide**2, -1, keepdims=True) + 1e-6)


def dot(a, b, dims):
    return lax.dot_general(a, b, ((dims[:1], dims[1:]), ((), ())), preferred_element_type=F32)


def aligned(start, size):
    return pl.ds(pl.multiple_of(start, 16), size)


class Place:
    def __init__(self):
        s = lax.axis_index("s")
        self.x, self.c, self.y = lax.div(s, 2), lax.rem(s, 2), lax.axis_index("r")

    def chip(self, d):
        return lax.rem(self.x + d, RING)

    def row(self, d):
        return lax.rem(self.y + d, RING)

    def at_x(self, d):
        return {"s": self.chip(d) * 2 + self.c}

    def at_y(self, d):
        return {"r": self.row(d)}

    def partner(self):
        return {"s": self.x * 2 + 1 - self.c}

    def greet(self):
        barrier = pltpu.get_barrier_semaphore()
        others = [self.at_x(d) for d in (1, 2, 3)] + [self.at_y(d) for d in (1, 2, 3)] + [self.partner()]
        for other in others:
            pl.semaphore_signal(barrier, inc=1, device_id=other, device_id_type=MESH)
        pl.semaphore_wait(barrier, len(others))


def remote(src, dst, send, recv, device):
    return pltpu.make_async_remote_copy(src_ref=src, dst_ref=dst, send_sem=send, recv_sem=recv, device_id=device, device_id_type=MESH)


class Fetch:
    COPIES = 17

    def __init__(self, place, shard, whole, send, recv):
        self.p, self.shard, self.whole, self.send, self.recv = place, shard, whole, send, recv
        self.rows = shard.shape[0]
        self.mine = lax.rem(place.y, 2)

    def part(self, d, half, quarter=None, ref=None):
        n = self.rows // 2
        start = half * n
        if quarter is not None:
            n //= 2
            start = start + quarter * n
        base = 0 if ref is not None else (self.p.chip(d) * 2 + self.p.c) * self.rows
        return (self.whole if ref is None else ref).at[aligned(base + start, n), :]

    def copy(self, k):
        p, h, o = self.p, self.mine, 1 - self.mine
        own = self.whole.at[aligned((p.x * 2 + p.c) * self.rows, self.rows), :]
        right, left, up, down, partner = p.at_x(1), p.at_x(3), p.at_y(1), p.at_y(3), p.partner()
        if k < 2:
            src, dst, to = self.part(0, h, ref=self.shard), self.part(0, h), (right, left)[k]
        elif k == 2:
            src, dst, to = self.shard, own, partner
        else:
            args, to = {
                3: ((3, h), up), 4: ((3, h, 0), right), 5: ((3, h), partner),
                6: ((1, h), down), 7: ((1, h, 1), left), 8: ((1, h), partner),
                9: ((3, o), partner), 10: ((1, o), partner),
                11: ((2, h, 0), up), 12: ((2, h, 0), partner),
                13: ((2, h, 1), down), 14: ((2, h, 1), partner),
                15: ((2, o, 0), partner), 16: ((2, o, 1), partner),
            }[k]
            src = dst = self.part(*args)
        return remote(src, dst, self.send.at[k], self.recv.at[k], to)

    def start(self, *ks):
        for k in ks:
            self.copy(k).start()

    def arrived(self, *ks):
        for k in ks:
            self.copy(k).wait_recv()

    def stage(self, n):
        if n == 0:
            self.start(0, 1, 2)
        elif n == 1:
            self.arrived(0)
            self.start(4, 3, 5)
            self.arrived(1)
            self.start(7, 6, 8)
        elif n == 2:
            self.arrived(4)
            self.start(11, 12)
            self.arrived(7)
            self.start(13, 14)
            self.arrived(3)
            self.start(9)
            self.arrived(6)
            self.start(10)
        elif n == 3:
            self.arrived(11)
            self.start(15)
            self.arrived(13)
            self.start(16)
        else:
            self.arrived(2, 5, 8, 9, 10, 12, 14, 15, 16)
            for k in range(self.COPIES):
                self.copy(k).wait_send()


def first_kernel(x_ref, *refs):
    shards, outs, scratch = refs[:3], refs[3:12], refs[12:]
    g1, u1, d1, d0, a_ref, gate_ref, up_ref, hid_ref, h_ref = outs
    wg, wu, wd, stage_g, stage_u, stage_d, send, recv, local = scratch
    place = Place()
    step = pl.program_id(0)
    here = (place.x * 2 + place.c)

    def fetch(layer, m):
        whole = ((wg, wu, wd), (g1, u1, d1))[layer][m]
        return Fetch(place, shards[m].at[layer], whole, send.at[layer, m], recv.at[layer, m])

    def own0(m):
        rows = shards[m].shape[1]
        return pltpu.make_async_copy(shards[m].at[0], (wg, wu, wd)[m].at[aligned(here * rows, rows), :], local.at[m])

    def own1_in(m):
        return pltpu.make_async_copy(shards[m].at[1], (stage_g, stage_u, stage_d)[m], local.at[3 + m])

    def own1_out(m):
        rows = shards[m].shape[1]
        return pltpu.make_async_copy((stage_g, stage_u, stage_d)[m], (g1, u1, d1)[m].at[aligned(here * rows, rows), :], local.at[6 + m])

    keep_d0 = pltpu.make_async_copy(wd, d0, local.at[9])

    @pl.when(step == 0)
    def _():
        place.greet()
        for m in range(3):
            fetch(0, m).stage(0)
        for m in range(3):
            own0(m).start()
            own1_in(m).start()
        for n in range(1, 5):
            for m in range(3):
                fetch(0, m).stage(n)
            if n == 1:
                for m in range(3):
                    fetch(1, m).stage(0)
        for m in range(3):
            own0(m).wait()
            own1_in(m).wait()
            own1_out(m).start()
        keep_d0.start()

    plan = {2: [(0, 1)], 3: [(1, 1)], 5: [(2, 1), (0, 2)], 6: [(1, 2), (0, 3)], 7: [(2, 2), (1, 3)]}
    for at, todo in plan.items():

        @pl.when(step == at)
        def _(todo=todo):
            for m, n in todo:
                fetch(1, m).stage(n)

    wide = x_ref[...].astype(F32)
    a_ref[...] = (wide * scale_of(wide)).astype(BF16)
    width = wg.shape[1] // 5

    def columns(j, _):
        at = pl.ds(pl.multiple_of(j * width, 128), width)
        gate = dot(a_ref[...], wg[:, at], (1, 0))
        up = dot(a_ref[...], wu[:, at], (1, 0))
        gate_ref[:, at] = gate
        up_ref[:, at] = up
        hid_ref[:, at] = (jax.nn.silu(gate) * up).astype(BF16)
        return 0

    lax.fori_loop(0, 5, columns, 0)
    h_ref[...] = x_ref[...] + dot(hid_ref[...], wd[...], (1, 0)).astype(BF16)

    @pl.when(step == pl.num_programs(0) - 1)
    def _():
        fetch(1, 2).stage(3)
        for m in range(3):
            fetch(1, m).stage(4)
            own1_out(m).wait()
        keep_d0.wait()


def first(x, weights, tile=256):
    t, d = x.shape
    ff = weights[0].shape[2]
    gd, du, dd = ((w.shape[1], w.shape[2]) for w in weights)

    def rows(width):
        return pl.BlockSpec((tile, width), lambda i: (i, 0))

    whole = [(d, ff), (d, ff), (ff, d)]
    return pl.pallas_call(
        first_kernel,
        name="first",
        grid=(t // tile,),
        in_specs=[rows(d), ANY, ANY, ANY],
        out_specs=[ANY] * 4 + [rows(d), rows(ff), rows(ff), rows(ff), rows(d)],
        out_shape=[jax.ShapeDtypeStruct(s, BF16) for s in whole]
        + [jax.ShapeDtypeStruct((ff, d), BF16), jax.ShapeDtypeStruct((t, d), BF16)]
        + [jax.ShapeDtypeStruct((t, ff), F32)] * 2
        + [jax.ShapeDtypeStruct((t, ff), BF16), jax.ShapeDtypeStruct((t, d), BF16)],
        scratch_shapes=[pltpu.VMEM(s, BF16) for s in whole]
        + [pltpu.VMEM(s, BF16) for s in (gd, du, dd)]
        + [pltpu.SemaphoreType.DMA((2, 3, Fetch.COPIES)), pltpu.SemaphoreType.DMA((2, 3, Fetch.COPIES)), pltpu.SemaphoreType.DMA((10,))],
        compiler_params=pltpu.CompilerParams(
            collective_id=0, has_side_effects=True, vmem_limit_bytes=VMEM_LIMIT, dimension_semantics=("arbitrary",)
        ),
        cost_estimate=pl.CostEstimate(flops=6 * t * d * ff, bytes_accessed=60_000_000, transcendentals=0),
    )(x, *weights)


def middle_kernel(h_ref, dy_ref, gate0_ref, up0_ref, g1, u1, d1, d0, a_ref, hid_ref, dg1_ref, du1_ref, dh_ref, dg0_ref, du0_ref):
    wide = h_ref[...].astype(F32)
    scale = scale_of(wide)
    a_ref[...] = (wide * scale).astype(BF16)
    ff = g1.shape[1]
    width = ff // 5

    def back(by_hid, gate, up):
        sig = jax.nn.sigmoid(gate)
        silu = gate * sig
        return by_hid * up * (sig * (1.0 + gate * (1.0 - sig))), by_hid * silu, silu * up

    def layer1(j, _):
        at = pl.ds(pl.multiple_of(j * width, 128), width)
        gate = dot(a_ref[...], g1[:, at], (1, 0))
        up = dot(a_ref[...], u1[:, at], (1, 0))
        by_hid = dot(dy_ref[...], d1[at, :], (1, 1)).astype(BF16).astype(F32)
        by_gate, by_up, hid = back(by_hid, gate, up)
        hid_ref[:, at] = hid.astype(BF16)
        dg1_ref[:, at] = by_gate.astype(BF16)
        du1_ref[:, at] = by_up.astype(BF16)
        return 0

    lax.fori_loop(0, 5, layer1, 0)
    by_a = dot(dg1_ref[...], g1[...], (1, 1)).astype(BF16) + dot(du1_ref[...], u1[...], (1, 1)).astype(BF16)
    by_a = by_a.astype(F32)
    along = jnp.sum(by_a * wide, -1, keepdims=True) * (1.0 / wide.shape[-1])
    by_h = by_a * scale - wide * (scale * scale * scale * along)
    dh_ref[...] = dy_ref[...] + by_h.astype(BF16)

    def layer0(j, _):
        at = pl.ds(pl.multiple_of(j * width, 128), width)
        by_hid = dot(dh_ref[...], d0[at, :], (1, 1)).astype(BF16).astype(F32)
        by_gate, by_up, _ = back(by_hid, gate0_ref[:, at], up0_ref[:, at])
        dg0_ref[:, at] = by_gate.astype(BF16)
        du0_ref[:, at] = by_up.astype(BF16)
        return 0

    lax.fori_loop(0, 5, layer0, 0)


def middle(h, dy, gate0, up0, g1, u1, d1, d0, tile=256):
    t, d = h.shape
    ff = g1.shape[1]

    def rows(width):
        return pl.BlockSpec((tile, width), lambda i: (i, 0))

    def fixed(w):
        return pl.BlockSpec(w.shape, lambda i: (0, 0), pipeline_mode=pl.Buffered(1))

    wide, narrow = jax.ShapeDtypeStruct((t, ff), BF16), jax.ShapeDtypeStruct((t, d), BF16)
    return pl.pallas_call(
        middle_kernel,
        name="middle",
        grid=(t // tile,),
        in_specs=[rows(d), rows(d), rows(ff), rows(ff)] + [fixed(w) for w in (g1, u1, d1, d0)],
        out_specs=[rows(d), rows(ff), rows(ff), rows(ff), rows(d), rows(ff), rows(ff)],
        out_shape=[narrow, wide, wide, wide, narrow, wide, wide],
        compiler_params=pltpu.CompilerParams(vmem_limit_bytes=VMEM_LIMIT, dimension_semantics=("arbitrary",)),
        cost_estimate=pl.CostEstimate(flops=12 * t * d * ff, bytes_accessed=120_000_000, transcendentals=0),
    )(h, dy, gate0, up0, g1, u1, d1, d0)


class Sum:
    COPIES = 11

    def __init__(self, place, x_first, theirs, came, mine, r1, r2, r3, final, out, send, recv, local):
        self.p, self.x_first = place, x_first
        self.theirs, self.came, self.mine, self.r1, self.r2, self.r3 = theirs, came, mine, r1, r2, r3
        self.final, self.out, self.send, self.recv, self.local = final, out, send, recv, local
        self.width = mine.shape[3]
        self.a, self.b = (place.chip, place.row) if x_first else (place.row, place.chip)
        self.at_a, self.at_b = (place.at_x, place.at_y) if x_first else (place.at_y, place.at_x)

    def block(self, d, half=None):
        t = self.a(d)
        w = self.width // 2
        cols = slice(None) if half is None else pl.ds(half * w, w)
        return self.mine.at[t, :, :, cols] if self.x_first else self.mine.at[:, t, :, cols]

    def cell(self, d):
        return self.mine.at[self.a(0), self.b(d)] if self.x_first else self.mine.at[self.b(d), self.a(0)]

    def slot(self, d):
        rows = self.final.shape[0]
        return self.out.at[aligned(self.p.y * rows, rows), :]

    def copy(self, k):
        if k == 0:
            src, dst, to = self.theirs, self.came, self.p.partner()
        elif k < 3:
            src, dst, to = self.block(2, k - 1), self.r1.at[k - 1], self.at_a((1, 3)[k - 1])
        elif k < 5:
            src, dst, to = self.block((1, 3)[k - 3]), self.r2.at[k - 3], self.at_a((1, 3)[k - 3])
        elif k < 8:
            src, dst, to = self.cell(k - 4), self.r3.at[k - 5], self.at_b(k - 4)
        else:
            src, dst, to = self.final, self.slot(0), self.p.at_y(k - 7)
        return remote(src, dst, self.send.at[k], self.recv.at[k], to)

    def keep(self):
        return pltpu.make_async_copy(self.final, self.slot(0), self.local)

    def start(self, *ks):
        for k in ks:
            self.copy(k).start()

    def wait(self, *ks):
        for k in ks:
            self.copy(k).wait()

    def add(self, into, *terms):
        total = into[...].astype(F32)
        for term in terms:
            total = total + term[...].astype(F32)
        into[...] = total.astype(BF16)

    def stage(self, n):
        if n == 0:
            self.start(0)
        elif n == 1:
            self.wait(0)

            def one(i, _):
                self.add(self.mine.at[i], self.came.at[i])
                return 0

            lax.fori_loop(0, RING, one, 0)
            self.start(1, 2)
        elif n == 2:
            self.wait(1)
            self.add(self.block(1, 0), self.r1.at[0])
            self.start(3)
            self.wait(2)
            self.add(self.block(3, 1), self.r1.at[1])
            self.start(4)
        elif n == 3:
            self.wait(3, 4)
            self.add(self.block(0), self.r2.at[0], self.r2.at[1])
            self.start(5, 6, 7)
        elif n == 4:
            self.wait(5, 6, 7)
            total = self.cell(0)[...].astype(F32)
            for d in range(3):
                total = total + self.r3[d].astype(F32)
            self.final[...] = total.astype(BF16)
            self.start(8, 9, 10)
            self.keep().start()
        else:
            self.wait(8, 9, 10)
            self.keep().wait()


X_FIRST = (True, False, True, True, False, True)


def last_kernel(hid1, dy, a1, dg1, du1, hid0, dh, a0, dg0, du0, *refs):
    outs, scratch = refs[:6], refs[6:]
    small, wide, theirs_d, came_d, mine_d, r1_d, r2_d, r3_d, final_d = scratch[:9]
    theirs_w, came_w, mine_w, r1_w, r2_w, r3_w, final_w, send, recv, local = scratch[9:]
    place = Place()
    chunk = wide.shape[2]
    jobs = [(dy, hid1), (a1, dg1), (a1, du1), (dh, hid0), (a0, dg0), (a0, du0)]

    def load_small(m):
        return pltpu.make_async_copy(jobs[m][0], small.at[{0: 0, 1: 1, 2: 1, 3: 0, 4: 1, 5: 1}[m]], local.at[6 + m])

    def load_wide(n):
        return pltpu.make_async_copy(jobs[n // RING][1].at[:, pl.ds(n % RING * chunk, chunk)], wide.at[n % 2], local.at[12 + n % 2])

    def summed(m):
        layer, kind = m // 3, m % 3
        if kind == 0:
            bufs = theirs_d, came_d, mine_d.at[layer], r1_d.at[layer], r2_d.at[layer], r3_d.at[layer], final_d.at[layer]
        else:
            w = layer * 2 + kind - 1
            bufs = theirs_w.at[w % 2], came_w.at[w % 2], mine_w.at[w % 3], r1_w.at[w], r2_w.at[w], r3_w.at[w], final_w.at[w]
        return Sum(place, X_FIRST[m], *bufs, outs[m], send.at[m], recv.at[m], local.at[m])

    def store(m, value, x, columns):
        sums = summed(m)
        rows = value.shape[0] // 2
        first, second = value[:rows].astype(BF16), value[rows:].astype(BF16)
        low = place.c == 0
        shape = (RING, rows // RING, value.shape[1])
        sums.mine[x, :, :, columns] = jnp.where(low, first, second).reshape(shape)
        sums.theirs[x, :, :, columns] = jnp.where(low, second, first).reshape(shape)

    def compute(m, j):
        lhs = small.at[{0: 0, 1: 1, 2: 1, 3: 0, 4: 1, 5: 1}[m]]
        n = (m * RING + j) % 2
        if m % 3 == 0:
            width = lhs.shape[1] // 2

            def half(i, _):
                at = pl.ds(pl.multiple_of(i * width, 128), width)
                store(m, dot(wide[n], lhs[:, at], (0, 0)), j, at)
                return 0

            lax.fori_loop(0, 2, half, 0)
        else:
            height = lhs.shape[1] // RING

            def chip(i, _):
                at = pl.ds(pl.multiple_of(i * height, 128), height)
                store(m, dot(lhs[:, at], wide[n], (0, 0)), i, pl.ds(j * chunk, chunk))
                return 0

            lax.fori_loop(0, RING, chip, 0)

    steps = 6 * RING
    load_small(0).start()
    load_wide(0).start()
    load_small(1).start()
    place.greet()
    todo = {}
    for m in range(6):
        for n, after in enumerate((0, 2, 4, 7, 9)):
            todo.setdefault(m * RING + RING - 1 + after, []).append((m, n))
    for t in range(steps):
        m, j = divmod(t, RING)
        if j == 0 and m != 2 and m != 5:
            load_small(m).wait()
        load_wide(t).wait()
        if t + 1 < steps:
            load_wide(t + 1).start()
        if t == RING:
            load_small(3).start()
        compute(m, j)
        if t == 3 * RING - 1:
            load_small(4).start()
        for k, n in todo.pop(t, []):
            summed(k).stage(n)
    for t in sorted(todo):
        for k, n in todo[t]:
            summed(k).stage(n)
    for m in range(6):
        summed(m).stage(5)


def last(hid1, dy, a1, dg1, du1, hid0, dh, a0, dg0, du0):
    t, ff = hid1.shape
    d = dy.shape[1]
    cores = 2 * RING
    tall, flat = (ff // cores, d), (d // cores, ff)
    cells_d, cells_w = (RING, RING, tall[0] // RING, d), (RING, RING, flat[0] // RING, ff)

    def received(count, cells):
        _, _, rows, width = cells
        return [
            pltpu.VMEM((count, 2, RING, rows, width // 2), BF16),
            pltpu.VMEM((count, 2, RING, rows, width), BF16),
            pltpu.VMEM((count, 3, rows, width), BF16),
            pltpu.VMEM((count, rows, width), BF16),
        ]

    return pl.pallas_call(
        last_kernel,
        name="last",
        in_specs=[ANY] * 10,
        out_specs=[ANY] * 6,
        out_shape=[jax.ShapeDtypeStruct(s, BF16) for s in (tall, flat, flat) * 2],
        scratch_shapes=[pltpu.VMEM((2, t, d), BF16), pltpu.VMEM((2, t, ff // RING), BF16)]
        + [pltpu.VMEM(cells_d, BF16), pltpu.VMEM(cells_d, BF16), pltpu.VMEM((2, *cells_d), BF16)]
        + received(2, cells_d)
        + [pltpu.VMEM((2, *cells_w), BF16), pltpu.VMEM((2, *cells_w), BF16), pltpu.VMEM((3, *cells_w), BF16)]
        + received(4, cells_w)
        + [pltpu.SemaphoreType.DMA((6, Sum.COPIES)), pltpu.SemaphoreType.DMA((6, Sum.COPIES)), pltpu.SemaphoreType.DMA((14,))],
        compiler_params=pltpu.CompilerParams(collective_id=1, has_side_effects=True, vmem_limit_bytes=VMEM_LIMIT),
        cost_estimate=pl.CostEstimate(flops=12 * t * d * ff, bytes_accessed=90_000_000, transcendentals=0),
    )(hid1, dy, a1, dg1, du1, hid0, dh, a0, dg0, du0)


def solution(mesh):
    def step(x, dy, *arrays):
        weights, m, v = (arrays[i : i + 3] for i in (0, 3, 6))
        g1, u1, d1, d0, a0, gate0, up0, hid0, h1 = first(x[0], weights)
        a1, hid1, dg1, du1, dh, dg0, du0 = middle(h1, dy[0], gate0, up0, g1, u1, d1, d0)
        down1, gate1, up1, down0, gate_0, up_0 = last(hid1, dy[0], a1, dg1, du1, hid0, dh, a0, dg0, du0)
        gradients = [jnp.stack(pair).astype(F32) for pair in ((gate_0, gate1), (up_0, up1), (down0, down1))]
        squares = lax.psum(sum(jnp.sum(g * g) for g in gradients), "s")
        gradients = clipped(gradients, squares, lax.psum(1, "s") * sum(g.size for g in gradients))
        new = [adamw(w.astype(F32), m, v, g) for w, m, v, g in zip(weights, m, v, gradients, strict=True)]
        return tuple(one[which] for which in range(3) for one in new)

    states, cut = P(("rep", "r", "s"), None, None), P(None, "s", None)
    return jax.shard_map(
        step,
        mesh=mesh,
        in_specs=(states, states) + (cut,) * 9,
        out_specs=(P("rep", "s", None),) * 9,
        check_vma=False,
    )
```

```python
import functools

import jax
import jax.numpy as jnp
from jax import lax
from jax.experimental import pallas as pl
from jax.experimental.pallas import tpu as pltpu
from jax.sharding import PartitionSpec as P

MESH = pl.DeviceIdType.MESH
BF16, F32 = jnp.bfloat16, jnp.float32
ANY = pl.BlockSpec(memory_space=pl.ANY)
VMEM_LIMIT = 67_000_000
PIECES = 10
RING = 4


def adamw(w, m, v, g):
    m = 0.9 * m + 0.1 * g
    v = 0.95 * v + 0.05 * g * g
    step = m * lax.rsqrt(v + 1e-8) + 0.1 * w
    return (w - 0.02 * step).astype(jnp.bfloat16), m, v


def clipped(gradients, sum_of_squares, count):
    factor = jnp.minimum(1.0, 0.5 * lax.rsqrt(sum_of_squares / count + 1e-30))
    return [g * factor for g in gradients]


def scale_of(wide):
    return lax.rsqrt(jnp.mean(wide**2, -1, keepdims=True) + 1e-6)


def dot(a, b, dims):
    return lax.dot_general(a, b, ((dims[:1], dims[1:]), ((), ())), preferred_element_type=F32)


def aligned(start, size):
    return pl.ds(pl.multiple_of(start, 16), size)


class Place:
    def __init__(self):
        s = lax.axis_index("s")
        self.x, self.c, self.y = lax.div(s, 2), lax.rem(s, 2), lax.axis_index("r")

    def chip(self, d):
        return lax.rem(self.x + d, RING)

    def row(self, d):
        return lax.rem(self.y + d, RING)

    def at_x(self, d):
        return {"s": self.chip(d) * 2 + self.c}

    def at_y(self, d):
        return {"r": self.row(d)}

    def partner(self):
        return {"s": self.x * 2 + 1 - self.c}

    def greet(self):
        barrier = pltpu.get_barrier_semaphore()
        others = [self.at_x(d) for d in range(1, RING)] + [self.at_y(d) for d in range(1, RING)] + [self.partner()]
        for other in others:
            pl.semaphore_signal(barrier, inc=1, device_id=other, device_id_type=MESH)
        pl.semaphore_wait(barrier, len(others))


def remote(src, dst, send, recv, device):
    return pltpu.make_async_remote_copy(src_ref=src, dst_ref=dst, send_sem=send, recv_sem=recv, device_id=device, device_id_type=MESH)


def TABLE(h, o, right, left, up, down, partner):
    before, beyond, far, low, high = 3, 1, 2, 0, 1
    lower, upper, far_low, far_high = (before, h), (beyond, h), (far, h, low), (far, h, high)
    return [
        (lower, up), ((before, h, low), right), (lower, partner),
        (upper, down), ((beyond, h, high), left), (upper, partner),
        ((before, o), partner), ((beyond, o), partner),
        (far_low, up), (far_low, partner), (far_high, down), (far_high, partner),
        ((far, o, low), partner), ((far, o, high), partner),
    ]


class Fetch:
    COPIES = 17

    def __init__(self, place, shard, whole, send, recv):
        self.p, self.shard, self.whole, self.send, self.recv = place, shard, whole, send, recv
        self.rows = shard.shape[0]
        self.mine = lax.rem(place.y, 2)

    def part(self, d, half, quarter=None, ref=None):
        n = self.rows // 2
        start = half * n
        if quarter is not None:
            n //= 2
            start = start + quarter * n
        base = 0 if ref is not None else (self.p.chip(d) * 2 + self.p.c) * self.rows
        return (self.whole if ref is None else ref).at[aligned(base + start, n), :]

    def copy(self, k):
        p, h, o = self.p, self.mine, 1 - self.mine
        own = self.whole.at[aligned((p.x * 2 + p.c) * self.rows, self.rows), :]
        right, left, up, down, partner = p.at_x(1), p.at_x(3), p.at_y(1), p.at_y(3), p.partner()
        if k < 2:
            src, dst, to = self.part(0, h, ref=self.shard), self.part(0, h), (right, left)[k]
        elif k == 2:
            src, dst, to = self.shard, own, partner
        else:
            args, to = TABLE(h, o, right, left, up, down, partner)[k - 3]
            src = dst = self.part(*args)
        return remote(src, dst, self.send.at[k], self.recv.at[k], to)

    def start(self, *ks):
        for k in ks:
            self.copy(k).start()

    def arrived(self, *ks):
        for k in ks:
            self.copy(k).wait_recv()

    def stage(self, n):
        if n == 0:
            self.start(0, 1, 2)
        elif n == 1:
            self.arrived(0)
            self.start(4, 3, 5)
            self.arrived(1)
            self.start(7, 6, 8)
        elif n == 2:
            self.arrived(4)
            self.start(11, 12)
            self.arrived(7)
            self.start(13, 14)
            self.arrived(3)
            self.start(9)
            self.arrived(6)
            self.start(10)
        elif n == 3:
            self.arrived(11)
            self.start(15)
            self.arrived(13)
            self.start(16)
        else:
            self.arrived(*(k for k in range(2, self.COPIES) if k not in (3, 4, 6, 7, 11, 13)))
            for k in range(self.COPIES):
                self.copy(k).wait_send()


def first_kernel(x_ref, *refs):
    shards, outs, scratch = refs[:3], refs[3:12], refs[12:]
    g1, u1, d1, d0, a_ref, gate_ref, up_ref, hid_ref, h_ref = outs
    wg, wu, wd, stage_g, stage_u, stage_d, send, recv, local = scratch
    place = Place()
    step = pl.program_id(0)
    here = (place.x * 2 + place.c)

    def fetch(layer, m):
        whole = ((wg, wu, wd), (g1, u1, d1))[layer][m]
        return Fetch(place, shards[m].at[layer], whole, send.at[layer, m], recv.at[layer, m])

    def own0(m):
        rows = shards[m].shape[1]
        return pltpu.make_async_copy(shards[m].at[0], (wg, wu, wd)[m].at[aligned(here * rows, rows), :], local.at[m])

    def own1_in(m):
        return pltpu.make_async_copy(shards[m].at[1], (stage_g, stage_u, stage_d)[m], local.at[3 + m])

    def own1_out(m):
        rows = shards[m].shape[1]
        return pltpu.make_async_copy((stage_g, stage_u, stage_d)[m], (g1, u1, d1)[m].at[aligned(here * rows, rows), :], local.at[6 + m])

    keep_d0 = pltpu.make_async_copy(wd, d0, local.at[9])

    @pl.when(step == 0)
    def _():
        place.greet()
        for m in range(3):
            fetch(0, m).stage(0)
        for m in range(3):
            own0(m).start()
            own1_in(m).start()
        for n in range(1, 5):
            for m in range(3):
                fetch(0, m).stage(n)
            if n == 1:
                for m in range(3):
                    fetch(1, m).stage(0)
        for m in range(3):
            own0(m).wait()
            own1_in(m).wait()
            own1_out(m).start()
        keep_d0.start()

    plan = {2: [(0, 1)], 3: [(1, 1)], 5: [(2, 1), (0, 2)], 6: [(1, 2), (0, 3)], 7: [(2, 2), (1, 3)]}
    for at, todo in plan.items():

        @pl.when(step == at)
        def _(todo=todo):
            for m, n in todo:
                fetch(1, m).stage(n)

    wide = x_ref[...].astype(F32)
    a_ref[...] = (wide * scale_of(wide)).astype(BF16)
    width = wg.shape[1] // PIECES

    def columns(j, _):
        at = pl.ds(pl.multiple_of(j * width, 128), width)
        gate = dot(a_ref[...], wg[:, at], (1, 0))
        up = dot(a_ref[...], wu[:, at], (1, 0))
        gate_ref[:, at] = gate
        up_ref[:, at] = up
        hid_ref[:, at] = (jax.nn.silu(gate) * up).astype(BF16)
        return _

    lax.fori_loop(0, PIECES, columns, 0, unroll=True)
    h_ref[...] = x_ref[...] + dot(hid_ref[...], wd[...], (1, 0)).astype(BF16)

    @pl.when(step == pl.num_programs(0) - 1)
    def _():
        fetch(1, 2).stage(3)
        for m in range(3):
            fetch(1, m).stage(4)
            own1_out(m).wait()
        keep_d0.wait()


def first(x, weights, tile=256):
    t, d = x.shape
    ff = weights[0].shape[2]
    gd, du, dd = ((w.shape[1], w.shape[2]) for w in weights)

    def rows(width):
        return pl.BlockSpec((tile, width), lambda i: (i, 0))

    whole = [(d, ff), (d, ff), (ff, d)]
    return pl.pallas_call(
        first_kernel,
        name="first",
        grid=(t // tile,),
        in_specs=[rows(d), ANY, ANY, ANY],
        out_specs=[ANY] * 4 + [rows(d), rows(ff), rows(ff), rows(ff), rows(d)],
        out_shape=[jax.ShapeDtypeStruct(s, BF16) for s in whole]
        + [jax.ShapeDtypeStruct((ff, d), BF16), jax.ShapeDtypeStruct((t, d), BF16)]
        + [jax.ShapeDtypeStruct((t, ff), F32)] * 2
        + [jax.ShapeDtypeStruct((t, ff), BF16), jax.ShapeDtypeStruct((t, d), BF16)],
        scratch_shapes=[pltpu.VMEM(s, BF16) for s in whole]
        + [pltpu.VMEM(s, BF16) for s in (gd, du, dd)]
        + [pltpu.SemaphoreType.DMA((2, 3, Fetch.COPIES)), pltpu.SemaphoreType.DMA((2, 3, Fetch.COPIES)), pltpu.SemaphoreType.DMA((10,))],
        compiler_params=pltpu.CompilerParams(
            collective_id=0, has_side_effects=True, vmem_limit_bytes=VMEM_LIMIT, dimension_semantics=("arbitrary",)
        ),
        cost_estimate=pl.CostEstimate(flops=6 * t * d * ff, bytes_accessed=60_000_000, transcendentals=0),
    )(x, *weights)


def middle_kernel(h_ref, dy_ref, gate0_ref, up0_ref, g1, u1, d1, d0, a_ref, hid_ref, dg1_ref, du1_ref, dh_ref, dg0_ref, du0_ref):
    wide = h_ref[...].astype(F32)
    scale = scale_of(wide)
    a_ref[...] = (wide * scale).astype(BF16)
    ff = g1.shape[1]
    width = ff // PIECES

    def back(by_hid, gate, up):
        sig = jax.nn.sigmoid(gate)
        silu = gate * sig
        return by_hid * up * (sig * (1.0 + gate * (1.0 - sig))), by_hid * silu, silu * up

    def layer1(j, _):
        at = pl.ds(pl.multiple_of(j * width, 128), width)
        gate = dot(a_ref[...], g1[:, at], (1, 0))
        up = dot(a_ref[...], u1[:, at], (1, 0))
        by_hid = dot(dy_ref[...], d1[at, :], (1, 1)).astype(BF16).astype(F32)
        by_gate, by_up, hid = back(by_hid, gate, up)
        hid_ref[:, at] = hid.astype(BF16)
        dg1_ref[:, at] = by_gate.astype(BF16)
        du1_ref[:, at] = by_up.astype(BF16)
        return _

    lax.fori_loop(0, PIECES, layer1, 0, unroll=True)
    by_a = dot(dg1_ref[...], g1[...], (1, 1)).astype(BF16) + dot(du1_ref[...], u1[...], (1, 1)).astype(BF16)
    by_a = by_a.astype(F32)
    along = jnp.sum(by_a * wide, -1, keepdims=True) * (1.0 / wide.shape[-1])
    by_h = by_a * scale - wide * (scale * scale * scale * along)
    dh_ref[...] = dy_ref[...] + by_h.astype(BF16)

    def layer0(j, _):
        at = pl.ds(pl.multiple_of(j * width, 128), width)
        by_hid = dot(dh_ref[...], d0[at, :], (1, 1)).astype(BF16).astype(F32)
        by_gate, by_up, hid = back(by_hid, gate0_ref[:, at], up0_ref[:, at])
        dg0_ref[:, at] = by_gate.astype(BF16)
        du0_ref[:, at] = by_up.astype(BF16)
        return _

    lax.fori_loop(0, PIECES, layer0, 0, unroll=True)


def middle(h, dy, gate0, up0, g1, u1, d1, d0, tile=256):
    t, d = h.shape
    ff = g1.shape[1]

    def rows(width):
        return pl.BlockSpec((tile, width), lambda i: (i, 0))

    def fixed(w):
        return pl.BlockSpec(w.shape, lambda i: (0, 0), pipeline_mode=pl.Buffered(1))

    wide, narrow = jax.ShapeDtypeStruct((t, ff), BF16), jax.ShapeDtypeStruct((t, d), BF16)
    return pl.pallas_call(
        middle_kernel,
        name="middle",
        grid=(t // tile,),
        in_specs=[rows(d), rows(d), rows(ff), rows(ff)] + [fixed(w) for w in (g1, u1, d1, d0)],
        out_specs=[rows(d), rows(ff), rows(ff), rows(ff), rows(d), rows(ff), rows(ff)],
        out_shape=[narrow, wide, wide, wide, narrow, wide, wide],
        compiler_params=pltpu.CompilerParams(vmem_limit_bytes=VMEM_LIMIT, dimension_semantics=("arbitrary",)),
        cost_estimate=pl.CostEstimate(flops=12 * t * d * ff, bytes_accessed=120_000_000, transcendentals=0),
    )(h, dy, gate0, up0, g1, u1, d1, d0)


class Sum:
    COPIES = 13

    def __init__(self, place, x_first, start, width, theirs, came, mine, r1, r2, t1, t2, final, out, send, recv, local):
        self.p, self.x_first, self.start_at, self.width = place, x_first, start, width
        self.theirs, self.came, self.mine, self.out = theirs, came, mine, out
        self.r1, self.r2, self.t1, self.t2, self.final = r1, r2, t1, t2, final
        self.send, self.recv, self.local = send, recv, local
        self.a, self.b = (place.chip, place.row) if x_first else (place.row, place.chip)
        self.at_a, self.at_b = (place.at_x, place.at_y) if x_first else (place.at_y, place.at_x)

    def columns(self, half=None):
        w = self.width // 2
        return pl.ds(self.start_at, self.width) if half is None else pl.ds(self.start_at + half * w, w)

    def narrow(self, ref, half=False):
        w = self.width // 2 if half else self.width
        at = self.start_at // 2 if half else self.start_at
        return ref.at[..., pl.ds(at, w)]

    def block(self, d, half=None):
        t, cols = self.a(d), self.columns(half)
        return self.mine.at[t, :, :, cols] if self.x_first else self.mine.at[:, t, :, cols]

    def cell(self, d, half=None):
        cols = self.columns(half)
        return self.mine.at[self.a(0), self.b(d), :, cols] if self.x_first else self.mine.at[self.b(d), self.a(0), :, cols]

    def slot(self, d, half=None):
        rows = self.final.shape[0]
        return self.out.at[aligned(self.p.row(d) * rows, rows), self.columns(half)]

    def copy(self, k):
        side = (k - 1) % 2
        a, b, y = self.at_a((1, 3)[side]), self.at_b((1, 3)[side]), self.p.at_y((1, 3)[side])
        near, far = (1, 3)[side], (3, 1)[side]
        if k == 0:
            src, dst, to = self.theirs.at[..., self.columns()], self.came.at[..., self.columns()], self.p.partner()
        elif k < 3:
            src, dst, to = self.block(2, side), self.narrow(self.r1.at[side], True), a
        elif k < 5:
            src, dst, to = self.block(near), self.narrow(self.r2.at[side]), a
        elif k < 7:
            src, dst, to = self.cell(2, side), self.narrow(self.t1.at[side], True), b
        elif k < 9:
            src, dst, to = self.cell(near), self.narrow(self.t2.at[side]), b
        elif k < 11:
            src, dst, to = self.narrow(self.final), self.slot(0), y
        else:
            src, dst, to = self.slot(far, side), self.slot(far, side), y
        return remote(src, dst, self.send.at[k], self.recv.at[k], to)

    def keep(self):
        return pltpu.make_async_copy(self.narrow(self.final), self.slot(0), self.local)

    def start(self, *ks):
        for k in ks:
            self.copy(k).start()

    def wait(self, *ks):
        for k in ks:
            self.copy(k).wait()

    def add(self, into, *terms, to=None):
        total = into[...].astype(F32)
        for term in terms:
            total = total + term[...].astype(F32)
        total = total.astype(BF16)
        (into if to is None else to)[...] = total
        return total

    def stage(self, n, squares):
        if n == 0:
            self.start(0)
        elif n == 1:
            self.wait(0)

            def one(i, _):
                self.add(self.mine.at[i, :, :, self.columns()], self.came.at[i, :, :, self.columns()])
                return _

            lax.fori_loop(0, RING, one, 0)
            self.start(1, 2)
        elif n == 2:
            self.wait(1)
            self.add(self.block(1, 0), self.narrow(self.r1.at[0], True))
            self.start(3)
            self.wait(2)
            self.add(self.block(3, 1), self.narrow(self.r1.at[1], True))
            self.start(4)
        elif n == 3:
            self.wait(3, 4)
            self.add(self.block(0), self.narrow(self.r2.at[0]), self.narrow(self.r2.at[1]))
            self.start(5, 6)
        elif n == 4:
            self.wait(5, 6)
            self.add(self.cell(1, 0), self.narrow(self.t1.at[0], True))
            self.add(self.cell(3, 1), self.narrow(self.t1.at[1], True))
            self.start(7, 8)
        elif n == 5:
            self.wait(7, 8)
            total = self.add(self.cell(0), self.narrow(self.t2.at[0]), self.narrow(self.t2.at[1]), to=self.narrow(self.final))
            self.start(9, 10)
            self.keep().start()
            total = total.astype(F32)
            squares[...] += jnp.full(squares.shape, jnp.sum(total * total), F32)
        elif n == 6:
            self.wait(9)
            self.start(11)
            self.wait(10)
            self.start(12)
        else:
            self.wait(11, 12)
            self.keep().wait()


class Everywhere:
    COPIES = 7

    def __init__(self, place, own, came, over_x, over_y, send, recv):
        self.p, self.own, self.came, self.over_x, self.over_y, self.send, self.recv = place, own, came, over_x, over_y, send, recv

    def copies(self, n):
        p = self.p
        if n == 0:
            return [remote(self.own, self.came, self.send.at[0], self.recv.at[0], p.partner())]
        slots, me, at = (self.over_x, p.x, p.at_x) if n == 1 else (self.over_y, p.y, p.at_y)
        return [remote(slots.at[me], slots.at[me], self.send.at[3 * n - 3 + d], self.recv.at[3 * n - 3 + d], at(d)) for d in range(1, RING)]

    def start(self, n):
        for copy in self.copies(n):
            copy.start()

    def end(self, n):
        for copy in self.copies(n):
            copy.wait()
        if n == 0:
            self.over_x[self.p.x] = self.own[...] + self.came[...]
            return None
        slots = self.over_x if n == 1 else self.over_y
        total = sum(slots[i] for i in range(RING))
        if n == 1:
            self.over_y[self.p.y] = total
        return total


TALL = (1, 3)
UNITS = []
for each in range(6):
    UNITS += [(each, 0, 1, True)] if each in TALL else [(each, share, 2, share > 0) for share in range(2)]
AFTER = (0, 2, 4, *range(7, 14, 2))


def last_kernel(a1, dg1, dy, hid1, du1, dh, hid0, a0, dg0, du0, *refs):
    outs, sum_ref, scratch = refs[:6], refs[6], refs[7:]
    small, wide = scratch[:2]
    bufs_d, bufs_w = scratch[2:10], scratch[10:18]
    own, own_came, over_x, over_y, send, recv, local, every_send, every_recv = scratch[18:]
    place = Place()
    chunk = wide.shape[2]
    wides = (dg1, hid1, du1, hid0, dg0, du0)
    smalls = {0: (a1, 0), 1: (dy, 1), 3: (dh, 1), 4: (a0, 0)}

    def load_small(m):
        src, slot = smalls[m]
        return pltpu.make_async_copy(src, small.at[slot], local.at[m])

    def load_wide(m, t):
        slot = lax.rem(t, 2)
        at = pl.ds(pl.multiple_of(lax.rem(t, RING) * chunk, 128), chunk)
        return pltpu.make_async_copy(wides[m].at[:, at], wide.at[slot], local.at[6 + slot])

    def tall_buffers(layer):
        return [buf.at[pick] for buf, pick in zip(bufs_d, (0, 0) + (layer,) * 6, strict=True)]

    def flat_buffers(m):
        w = (m + 1) // 2
        return [buf.at[pick] for buf, pick in zip(bufs_w, (w % 2, w % 2) + (w,) * 6, strict=True)]

    def unit(k):
        m, share, shares, x_first = UNITS[k]
        bufs = tall_buffers(m // 3) if m in TALL else flat_buffers(m)
        width = bufs[2].shape[3] // shares
        return Sum(place, x_first, share * width, width, *bufs, outs[m], send.at[k], recv.at[k], local.at[8 + k])

    def store(bufs, value, x, columns):
        theirs, _, mine = bufs[:3]
        rows = value.shape[0] // 2
        first, second = value[:rows].astype(BF16), value[rows:].astype(BF16)
        low = place.c == 0
        shape = (RING, rows // RING, value.shape[1])
        mine[x, :, :, columns] = jnp.where(low, first, second).reshape(shape)
        theirs[x, :, :, columns] = jnp.where(low, second, first).reshape(shape)

    def tall(m, j, slot):
        lhs, bufs = small.at[1], tall_buffers(m // 3)
        width = lhs.shape[1] // 2
        for i in range(2):
            at = pl.ds(i * width, width)
            store(bufs, dot(wide[slot], lhs[:, at], (0, 0)), j, at)

    def flat(m, j, slot):
        lhs, bufs = small.at[0], flat_buffers(m)
        height = lhs.shape[1] // RING
        columns = pl.ds(pl.multiple_of(j * chunk, 128), chunk)
        for i in range(RING):
            store(bufs, dot(lhs[:, i * height : (i + 1) * height], wide[slot], (0, 0)), i, columns)

    steps = 6 * RING
    load_small(0).start()
    load_wide(0, 0).start()
    load_small(1).start()
    own[...] = jnp.zeros_like(own)
    place.greet()
    todo = {}
    for k, (m, share, shares, _) in enumerate(UNITS):
        ready = m * RING + (RING * (share + 1)) // shares - 1
        for n, after in enumerate(AFTER):
            todo.setdefault(ready + after, []).append((k, n))

    def work(t, carry):
        m, j, slot = t // RING, t % RING, t % 2
        for first in smalls:

            @pl.when(t == first * RING)
            def _(first=first):
                load_small(first).wait()

        load_wide(0, t).wait()
        for each in range(6):

            @pl.when((t + 1) // RING == each)
            def _(each=each):
                load_wide(each, t + 1).start()

        for each, free in ((3, 2), (4, 3)):

            @pl.when(t == free * RING)
            def _(each=each):
                load_small(each).start()

        is_tall = (m == TALL[0]) | (m == TALL[1])

        @pl.when(is_tall)
        def _():
            tall(m, j, slot)

        @pl.when(jnp.logical_not(is_tall))
        def _():
            flat(m, j, slot)

        for at in sorted(todo):
            if at < steps:

                @pl.when(t == at)
                def _(at=at):
                    for k, n in todo[at]:
                        unit(k).stage(n, own)

        return carry

    lax.fori_loop(0, steps, work, 0)
    rest = [each for t in sorted(todo) if t >= steps for each in todo[t]]
    for k, n in rest:
        if n < 6:
            unit(k).stage(n, own)
    every = Everywhere(place, own, own_came, over_x, over_y, every_send, every_recv)
    every.start(0)
    for k, n in rest:
        if n == 6:
            unit(k).stage(n, own)
    every.end(0)
    every.start(1)
    every.end(1)
    every.start(2)
    for k in range(len(UNITS)):
        unit(k).stage(7, own)
    sum_ref[...] = every.end(2)


def last(*operands):
    a1, dg1 = operands[:2]
    t, d = a1.shape
    ff = dg1.shape[1]
    cores = 2 * RING
    tall, flat = (ff // cores, d), (d // cores, ff)
    cells_d, cells_w = (RING, RING, tall[0] // RING, d), (RING, RING, flat[0] // RING, ff)

    def buffers(theirs, mine, count, cells):
        _, _, rows, width = cells
        return [
            pltpu.VMEM((theirs, *cells), BF16),
            pltpu.VMEM((theirs, *cells), BF16),
            pltpu.VMEM((mine, *cells), BF16),
            pltpu.VMEM((count, 2, RING, rows, width // 2), BF16),
            pltpu.VMEM((count, 2, RING, rows, width), BF16),
            pltpu.VMEM((count, 2, rows, width // 2), BF16),
            pltpu.VMEM((count, 2, rows, width), BF16),
            pltpu.VMEM((count, rows, width), BF16),
        ]

    units = len(UNITS)
    number = (8, 128)
    return pl.pallas_call(
        last_kernel,
        name="last",
        in_specs=[ANY] * 10,
        out_specs=[ANY] * 6 + [pl.BlockSpec(memory_space=pltpu.VMEM)],
        out_shape=[jax.ShapeDtypeStruct(s, BF16) for s in (flat, tall, flat, tall, flat, flat)] + [jax.ShapeDtypeStruct(number, F32)],
        scratch_shapes=[pltpu.VMEM((2, t, d), BF16), pltpu.VMEM((2, t, ff // RING), BF16)]
        + buffers(1, 2, 2, cells_d)
        + buffers(2, 4, 4, cells_w)
        + [pltpu.VMEM(number, F32), pltpu.VMEM(number, F32), pltpu.VMEM((RING, *number), F32), pltpu.VMEM((RING, *number), F32)]
        + [pltpu.SemaphoreType.DMA((units, Sum.COPIES)), pltpu.SemaphoreType.DMA((units, Sum.COPIES)), pltpu.SemaphoreType.DMA((8 + units,))]
        + [pltpu.SemaphoreType.DMA((Everywhere.COPIES,)), pltpu.SemaphoreType.DMA((Everywhere.COPIES,))],
        compiler_params=pltpu.CompilerParams(collective_id=1, has_side_effects=True, vmem_limit_bytes=VMEM_LIMIT),
        cost_estimate=pl.CostEstimate(flops=12 * t * d * ff, bytes_accessed=90_000_000, transcendentals=0),
    )(*operands)


def solution(mesh):
    def step(x, dy, *arrays):
        weights, m, v = (arrays[i : i + 3] for i in (0, 3, 6))
        g1, u1, d1, d0, a0, gate0, up0, hid0, h1 = first(x[0], weights)
        a1, hid1, dg1, du1, dh, dg0, du0 = middle(h1, dy[0], gate0, up0, g1, u1, d1, d0)
        gate1, down1, up1, down0, gate_0, up_0, squares = last(a1, dg1, dy[0], hid1, du1, dh, hid0, a0, dg0, du0)
        gradients = [jnp.stack(pair).astype(F32) for pair in ((gate_0, gate1), (up_0, up1), (down0, down1))]
        gradients = clipped(gradients, squares[0, 0], lax.psum(1, "s") * sum(g.size for g in gradients))
        new = [adamw(w.astype(F32), m, v, g) for w, m, v, g in zip(weights, m, v, gradients, strict=True)]
        return tuple(one[which] for which in range(3) for one in new)

    states, cut = P(("rep", "r", "s"), None, None), P(None, "s", None)
    return jax.shard_map(
        step,
        mesh=mesh,
        in_specs=(states, states) + (cut,) * 9,
        out_specs=(P("rep", "s", None),) * 9,
        check_vma=False,
    )
```
